32 devices in a mesh: dp: 8 (over y, x, core), tensor: 4 (over z).
Axes of the slice: x: 2, y: 2, z: 4, core: 2. Of those that a mesh axis runs over, the one named last changes fastest.
Arguments:
- attn_out: bfloat16 [3072, 4096], P('dp', 'tensor'), may hold values from -24 to 24
- out_grad: bfloat16 [3072, 4096], P('dp', 'tensor'), may hold values from -6 to 6
- proj_in: bfloat16 [64, 4096], P(None, 'tensor'), may hold values from -0.09375 to 0.09375
- proj_out: bfloat16 [64, 4096], P(None, 'tensor'), may hold values from -0.09375 to 0.09375
- targets: float32 [256, 64, 64], P(None, 'tensor'), may hold values from -6 to 6
Outputs:
- scores: float32 [48, 256], P('dp')
The draws below stay inside these ranges and needn't reach their ends.
All inputs are finite; a program needn't handle non-finite values.
Results may differ from the reference program's by a relative error of at most 0.0015.
Values sent between devices are 32-bit elements; how exact they have to be, the bound alone decides.
A program may use at most 64 MiB of HBM per device.

```python
import math
import jax
import jax.numpy as jnp
from jax import lax

D = 4096
R = 64
LEN = 64
NT = 256
TOKENS = 3072
SAMPLES = 48


def draw_attn_out(key, part):
    key_base, key_sample = jax.random.split(key, 2)
    positions = jnp.arange(TOKENS, dtype=jnp.float32)
    trend = jnp.sqrt(1.0 + 2.0 * positions / (TOKENS - 1))
    sample_scale = jnp.exp(jax.random.uniform(key_sample, (TOKENS // LEN,), minval=0.0, maxval=0.5 * math.log(10.0)))
    row_scale = trend * jnp.repeat(sample_scale, LEN)
    base = jax.random.truncated_normal(key_base, -4.0, 4.0, (TOKENS, D))
    return (base * row_scale[:, None]).astype(jnp.bfloat16)


def block_levels(key, dims, shards, smallest, high):
    gain, own = 1.0, jax.random.fold_in(key, 6)
    for position, shards_of in shards:
        draws = jnp.exp(jax.random.uniform(jax.random.fold_in(own, position), (shards_of,), jnp.float32, smallest / len(shards), high / len(shards)))
        gain = gain * jnp.repeat(draws, dims[position] // shards_of).reshape([-1 if axis == position else 1 for axis in range(len(dims))])
    return gain


def normal_values(rng, shape, scale, limit, cuts=(), kind=jnp.bfloat16):
    level = block_levels(rng, shape, cuts, -0.22, 0.18) if cuts else 1.0
    values = jax.random.normal(rng, shape, jnp.float32) * scale * level
    return jnp.minimum(jnp.maximum(values, -limit), limit).astype(kind)


def setup_inputs(seed: int = 0) -> dict:
    streams_of = jax.random.split(jax.random.key(seed), 6)
    attn_out = draw_attn_out(jax.random.fold_in(streams_of[5], 71), 0)
    out_grad = normal_values(streams_of[1], (TOKENS, D), 1.0, 6.0, ((0, 8), (1, 4)))
    proj_in = normal_values(streams_of[2], (R, D), D ** -0.5, 0.09375, ((1, 4),))
    proj_out = normal_values(streams_of[3], (R, D), D ** -0.5, 0.09375, ((1, 4),))
    targets = normal_values(streams_of[4], (NT, R, R), 1.0, 6.0, ((1, 4),), jnp.float32)
    return dict(attn_out=attn_out, out_grad=out_grad, proj_in=proj_in, proj_out=proj_out, targets=targets)


def reference(attn_out, out_grad, proj_in, proj_out, targets):
    highest = lax.Precision.HIGHEST
    inputs_low = jnp.einsum('td,rd->tr', attn_out.astype(jnp.float32), proj_in.astype(jnp.float32), preferred_element_type=jnp.float32)
    grads_low = jnp.einsum('td,rd->tr', out_grad.astype(jnp.float32), proj_out.astype(jnp.float32), preferred_element_type=jnp.float32)
    sample_grads = jnp.einsum('sti,sto->sio', inputs_low.reshape(SAMPLES, LEN, R), grads_low.reshape(SAMPLES, LEN, R), precision=highest).reshape(SAMPLES, R * R)
    damping = 0.5 * jnp.sum(sample_grads * sample_grads) / (SAMPLES * R * R) + 1e-06
    fisher = jnp.dot(sample_grads.T, sample_grads, precision=highest) / SAMPLES
    fisher = fisher + damping * jnp.eye(R * R, dtype=jnp.float32)
    target_rows = targets.reshape(NT, R * R)
    solved = jnp.linalg.solve(fisher, target_rows.T)
    return jnp.dot(sample_grads, solved, precision=highest)
```

```python
import functools

import jax
import jax.numpy as jnp
from jax import lax
from jax.experimental import pallas as pl
from jax.experimental.pallas import tpu as pltpu
from jax.sharding import PartitionSpec as P

LEN = 64
MESH = pl.DeviceIdType.MESH
NT = (((1,), (1,)), ((), ()))
NN = (((1,), (0,)), ((), ()))

damping_ratio = 0.5
epsilon = 1e-06


def dot32(left, right, dims):
    return lax.dot_general(
        left, right, dims, precision=lax.Precision.HIGHEST, preferred_element_type=jnp.float32
    )


def invert(system, n, width, ref):
    rows = lax.broadcasted_iota(jnp.int32, (n, 2 * width), 0)
    lanes = lax.broadcasted_iota(jnp.int32, (n, 2 * width), 1)
    work = jnp.where(lanes == rows + width, 1.0, system)
    if n <= width and n <= 64:
        for k in range(n):
            column = jnp.broadcast_to(work[:, k : k + 1], work.shape)
            row = work[k : k + 1, :] / column[k : k + 1, :]
            work = jnp.where(rows == k, row, work - column * row)
        return pltpu.roll(work, width, 1)[:, :width]
    ref[...] = work

    def step(k, carry):
        column = jnp.sum(jnp.where(lanes == k, ref[...], 0.0), axis=1, keepdims=True)
        pivot = jnp.sum(jnp.where(rows[:, :1] == k, column, 0.0))
        row = ref[pl.ds(k, 1), :] / pivot
        ref[...] = jnp.where(rows == k, row, ref[...] - column * row)
        return carry

    lax.fori_loop(0, n, step, 0)
    return ref[:, width:]


def kernel(
    n_dp, n_tp, pack,
    attn, ograd, proj_in, proj_out, targets, out,
    a_buf, g_buf, wi, wo, t_buf, t_flat, rs_out, rs_in, a2a_out, a2a_in, s_all,
    gram, cz, c_all, c_mat, inv_ref,
    load_sem, rs_s, rs_r, a2a_s, a2a_r, ag_s, ag_r, gr_s, gr_r, cz_s, cz_r, ca_s, ca_r,
):
    d, z = lax.axis_index("dp"), lax.axis_index("tensor")
    share = rs_out.shape[1]
    rank = proj_in.shape[0]
    per = s_all.shape[0] // n_dp
    n = s_all.shape[0]
    half = s_all.shape[1]
    slots = a2a_out.shape[1] // half

    def each(count, body):
        if count <= 16:
            for k in range(1, count):
                body(k)
        else:
            lax.fori_loop(1, count, lambda k, c: (body(k), c)[1], 0)

    def z_peer(k):
        return lax.rem(z + k, n_tp)

    def d_peer(k):
        return lax.rem(d + k, n_dp)

    barrier = pltpu.get_barrier_semaphore()
    each(n_tp, lambda k: pl.semaphore_signal(barrier, inc=1, device_id=(d, z_peer(k)), device_id_type=MESH))
    each(n_dp, lambda k: pl.semaphore_signal(barrier, inc=1, device_id=(d_peer(k), z), device_id_type=MESH))

    load_pi = pltpu.make_async_copy(proj_in, wi.at[pl.ds(0, rank)], load_sem.at[0])
    load_po = pltpu.make_async_copy(proj_out, wo.at[pl.ds(rank, rank)], load_sem.at[1])
    load_pi.start()
    load_po.start()
    order = [k for k in (2, 3, 1) if k < n_tp] + list(range(4, n_tp)) + [0]
    loads = {}
    for k in order:
        rows = pl.ds(pl.multiple_of(z_peer(k) * share, share), share)
        loads[k] = (
            pltpu.make_async_copy(attn.at[rows], a_buf.at[k], load_sem.at[3 + 2 * k]),
            pltpu.make_async_copy(ograd.at[rows], g_buf.at[k], load_sem.at[4 + 2 * k]),
        )
        for copy in loads[k]:
            copy.start()
    load_t = pltpu.make_async_copy(targets, t_buf, load_sem.at[2])
    load_t.start()
    wi[pl.ds(rank, rank), :] = jnp.zeros((rank, wi.shape[1]), wi.dtype)
    wo[pl.ds(0, rank), :] = jnp.zeros((rank, wo.shape[1]), wo.dtype)
    load_pi.wait()
    load_po.wait()

    def z_copy(src, dst, send, recv, k):
        return pltpu.make_async_remote_copy(
            src_ref=src, dst_ref=dst, send_sem=send, recv_sem=recv,
            device_id=(d, z_peer(k)), device_id_type=MESH,
        )

    def d_copy(src, dst, send, recv, k):
        return pltpu.make_async_remote_copy(
            src_ref=src, dst_ref=dst, send_sem=send, recv_sem=recv,
            device_id=(d_peer(k), z), device_id_type=MESH,
        )

    sends = []

    def rs_copy(k):
        return z_copy(rs_out.at[k], rs_in.at[z], rs_s.at[k], rs_r.at[z], k)

    for position, k in enumerate(order):
        for copy in loads[k]:
            copy.wait()
        part = lax.dot_general(a_buf[k], wi[...], NT, preferred_element_type=jnp.float32)
        part = part + lax.dot_general(g_buf[k], wo[...], NT, preferred_element_type=jnp.float32)
        if k:
            rs_out[k] = part
            if position == 0:
                pl.semaphore_wait(barrier, n_tp + n_dp - 2)
            copy = rs_copy(k)
            copy.start()
            sends.append(copy)
        else:
            rs_in[z] = part

    load_t.wait()
    for r in range(half):
        t_flat[:, pl.ds(r * 2 * rank, 2 * rank)] = jnp.concatenate(
            [t_buf[:, r, :], t_buf[:, r + half, :]], axis=1
        )

    def wait_z(buf, recv):
        for k in range(1, n_tp):
            src = lax.rem(z + n_tp - k, n_tp)
            pltpu.make_async_remote_copy(
                src_ref=buf.at[src], dst_ref=buf.at[src], send_sem=recv.at[src], recv_sem=recv.at[src],
                device_id=(d, src), device_id_type=MESH,
            ).wait_recv()

    wait_z(rs_in, rs_r)
    low = rs_in[0]
    for src in range(1, n_tp):
        low = low + rs_in[src]
    lanes = lax.broadcasted_iota(jnp.int32, low.shape, 1)
    grads = jnp.where(lanes < rank, pltpu.roll(low, rank, 1), low)
    inputs_t = low.T[:rank]
    token = lax.broadcasted_iota(jnp.int32, inputs_t.shape, 1) + z * share
    first = (z * share) // LEN
    left = jnp.concatenate(
        [
            jnp.where((token >= (first + s) * LEN) & (token < (first + s + 1) * LEN), inputs_t, 0.0)
            for s in range(slots)
        ],
        axis=0,
    )
    prods = dot32(left, grads, NN)
    low_lanes = lax.broadcasted_iota(jnp.int32, (half, 2 * rank), 1) < rank
    for q in range(n_tp):
        for s in range(slots):
            base = s * rank + q * 2 * half
            a2a_out[q, s * half : (s + 1) * half, :] = jnp.where(
                low_lanes, prods[base : base + half], prods[base + half : base + 2 * half]
            )
    for k in range(1, n_tp):
        copy = z_copy(a2a_out.at[z_peer(k)], a2a_in.at[z], a2a_s.at[k], a2a_r.at[z], k)
        copy.start()
        sends.append(copy)
    a2a_in[z] = a2a_out[z]
    wait_z(a2a_in, a2a_r)
    mine = [None] * per
    for src in range(n_tp):
        for s in range(slots):
            sample = (src * share) // LEN + s
            if sample * LEN >= (src + 1) * share:
                continue
            term = a2a_in[src, s * half : (s + 1) * half, :]
            mine[sample] = term if mine[sample] is None else mine[sample] + term
    for sample in range(per):
        s_all[d * per + sample] = mine[sample]

    own = pl.ds(d * per, per)

    def ag_copy(k):
        return d_copy(s_all.at[own], s_all.at[own], ag_s.at[k], ag_r.at[d], k)

    each(n_dp, lambda k: ag_copy(k).start())

    own_flat = jnp.concatenate([s_all[own, r, :] for r in range(half)], axis=1)
    cz[z, pl.ds(0, per), :] = dot32(own_flat, t_flat[...], NT)
    if cz.shape[1] > per:
        cz[z, pl.ds(per, cz.shape[1] - per), :] = jnp.zeros((cz.shape[1] - per, cz.shape[2]), jnp.float32)
    for k in range(1, n_tp):
        copy = z_copy(cz.at[z], cz.at[z], cz_s.at[k], cz_r.at[z], k)
        copy.start()
        sends.append(copy)

    def wait_ag(k):
        src = lax.rem(d + n_dp - k, n_dp)
        block = s_all.at[pl.ds(src * per, per)]
        pltpu.make_async_remote_copy(
            src_ref=block, dst_ref=block, send_sem=ag_r.at[src], recv_sem=ag_r.at[src],
            device_id=(src, z), device_id_type=MESH,
        ).wait_recv()

    each(n_dp, wait_ag)
    flat = jnp.concatenate([s_all[:, r, :] for r in range(half)], axis=1)
    width = gram.shape[2]
    if pack:
        pad = jnp.zeros((width // 2 - n, flat.shape[1]), jnp.float32)
        full = dot32(flat, jnp.concatenate([flat, pad, flat, pad], axis=0), NT)
        g_lanes = lax.broadcasted_iota(jnp.int32, (n // 2, width), 1)
        gram[z] = jnp.where(g_lanes < width // 2, full[: n // 2], full[n // 2 :])
    else:
        gram[z] = dot32(flat, flat, NT)
    for k in range(1, n_tp):
        copy = z_copy(gram.at[z], gram.at[z], gr_s.at[k], gr_r.at[z], k)
        copy.start()
        sends.append(copy)

    wait_z(cz, cz_r)
    total = cz[0]
    for src in range(1, n_tp):
        total = total + cz[src]
    c_all[d] = total

    def ca_copy(k):
        return d_copy(c_all.at[d], c_all.at[d], ca_s.at[k], ca_r.at[d], k)

    each(n_dp, lambda k: ca_copy(k).start())

    wait_z(gram, gr_r)
    g_sum = gram[0]
    for src in range(1, n_tp):
        g_sum = g_sum + gram[src]
    if pack:
        g_sum = jnp.concatenate([g_sum, pltpu.roll(g_sum, width // 2, 1)], axis=0)
        system_width = width // 2
        wide = g_sum
    else:
        system_width = width
        wide = jnp.concatenate([g_sum, jnp.zeros_like(g_sum)], axis=1)
    g_rows = lax.broadcasted_iota(jnp.int32, wide.shape, 0)
    g_cols = lax.broadcasted_iota(jnp.int32, wide.shape, 1)
    wide = jnp.where(g_cols < n, wide, 0.0)
    diagonal = g_rows == g_cols
    trace = jnp.sum(jnp.where(diagonal, wide, 0.0))
    damping = damping_ratio * trace / (n * rank * rank) + epsilon
    system = wide / n + jnp.where(diagonal, damping, 0.0)
    inverse = invert(system, n, system_width, inv_ref)
    inv_ref[:, pl.ds(0, system_width)] = inverse

    def wait_ca(k):
        src = lax.rem(d + n_dp - k, n_dp)
        block = c_all.at[src]
        pltpu.make_async_remote_copy(
            src_ref=block, dst_ref=block, send_sem=ca_r.at[src], recv_sem=ca_r.at[src],
            device_id=(src, z), device_id_type=MESH,
        ).wait_recv()

    each(n_dp, wait_ca)
    for q in range(n_dp):
        c_mat[q * per : (q + 1) * per, :] = c_all[q, :per, :]
    weights = jnp.concatenate([inv_ref[pl.ds(d * per + i, 1), :] for i in range(per)], axis=0)[:, :n]
    out[...] = dot32(weights, c_mat[...], NN)

    for copy in sends:
        copy.wait_send()
    each(n_dp, lambda k: ag_copy(k).wait_send())
    each(n_dp, lambda k: ca_copy(k).wait_send())


def shards(n_dp, n_tp, attn_out, out_grad, proj_in, proj_out, targets):
    tokens, model = attn_out.shape
    rank = proj_in.shape[0]
    n_targets, part_width, _ = targets.shape
    per = tokens // LEN
    n = per * n_dp
    share = tokens // n_tp
    half = part_width // 2
    slots = max(-(-((q + 1) * share) // LEN) - (q * share) // LEN for q in range(n_tp))
    pack = n <= rank and n % 16 == 0 and rank == 64
    padded = -(-per // 8) * 8
    gram_shape = (n_tp, n // 2, 2 * rank) if pack else (n_tp, n, n)
    inv_width = 2 * rank if pack else 2 * n
    f32, dma = jnp.float32, pltpu.SemaphoreType.DMA
    any_spec = pl.BlockSpec(memory_space=pl.ANY)
    return pl.pallas_call(
        functools.partial(kernel, n_dp, n_tp, pack),
        out_shape=jax.ShapeDtypeStruct((per, n_targets), f32),
        in_specs=[any_spec] * 5,
        out_specs=pl.BlockSpec(memory_space=pltpu.VMEM),
        scratch_shapes=[
            pltpu.VMEM((n_tp, share, model), attn_out.dtype),
            pltpu.VMEM((n_tp, share, model), out_grad.dtype),
            pltpu.VMEM((2 * rank, model), proj_in.dtype),
            pltpu.VMEM((2 * rank, model), proj_out.dtype),
            pltpu.VMEM(targets.shape, f32),
            pltpu.VMEM((n_targets, part_width * rank), f32),
            pltpu.VMEM((n_tp, share, 2 * rank), f32),
            pltpu.VMEM((n_tp, share, 2 * rank), f32),
            pltpu.VMEM((n_tp, slots * half, 2 * rank), f32),
            pltpu.VMEM((n_tp, slots * half, 2 * rank), f32),
            pltpu.VMEM((n, half, 2 * rank), f32),
            pltpu.VMEM(gram_shape, f32),
            pltpu.VMEM((n_tp, padded, n_targets), f32),
            pltpu.VMEM((n_dp, padded, n_targets), f32),
            pltpu.VMEM((n, n_targets), f32),
            pltpu.VMEM((n, inv_width), f32),
            dma((3 + 2 * n_tp,)),
        ]
        + [dma((n_tp,))] * 4
        + [dma((n_dp,))] * 2
        + [dma((n_tp,))] * 4
        + [dma((n_dp,))] * 2,
        compiler_params=pltpu.CompilerParams(
            collective_id=0, has_side_effects=True, vmem_limit_bytes=60 * 1024 * 1024
        ),
    )(attn_out, out_grad, proj_in, proj_out, targets)


def solution(mesh):
    in_specs = (
        P("dp", "tensor"),
        P("dp", "tensor"),
        P(None, "tensor"),
        P(None, "tensor"),
        P(None, "tensor", None),
    )
    return jax.shard_map(
        functools.partial(shards, mesh.shape["dp"], mesh.shape["tensor"]),
        mesh=mesh, in_specs=in_specs, out_specs=P("dp", None), check_vma=False,
    )
```

```python
import functools

import jax
import jax.numpy as jnp
from jax import lax
from jax.experimental import pallas as pl
from jax.experimental.pallas import tpu as pltpu
from jax.sharding import PartitionSpec as P

LEN = 64
MESH = pl.DeviceIdType.MESH
NT = (((1,), (1,)), ((), ()))
NN = (((1,), (0,)), ((), ()))

damping_ratio = 0.5
epsilon = 1e-06


def dot32(left, right, dims):
    return lax.dot_general(
        left, right, dims, precision=lax.Precision.HIGHEST, preferred_element_type=jnp.float32
    )


def invert(system, n, width, ref):
    rows = lax.broadcasted_iota(jnp.int32, (n, 2 * width), 0)
    lanes = lax.broadcasted_iota(jnp.int32, (n, 2 * width), 1)
    work = jnp.where(lanes == rows + width, 1.0, system)
    if n <= width and n <= 64 and n % 2 == 0:
        for k in range(0, n, 2):
            one = jnp.broadcast_to(work[:, k : k + 1], work.shape)
            two = jnp.broadcast_to(work[:, k + 1 : k + 2], work.shape)
            top, low = work[k : k + 1, :], work[k + 1 : k + 2, :]
            scale = 1.0 / one[k : k + 1, :]
            cross, ratio = two[k : k + 1, :], one[k + 1 : k + 2, :] * scale
            second = (low - ratio * top) / (two[k + 1 : k + 2, :] - ratio * cross)
            first = (top - cross * second) * scale
            rest = work - one * first - two * second
            work = jnp.where(rows == k, first, jnp.where(rows == k + 1, second, rest))
        return pltpu.roll(work, width, 1)[:, :width]
    ref[...] = work

    def step(k, carry):
        column = jnp.sum(jnp.where(lanes == k, ref[...], 0.0), axis=1, keepdims=True)
        pivot = jnp.sum(jnp.where(rows[:, :1] == k, column, 0.0))
        row = ref[pl.ds(k, 1), :] / pivot
        ref[...] = jnp.where(rows == k, row, ref[...] - column * row)
        return carry

    lax.fori_loop(0, n, step, 0)
    return ref[:, width:]


def kernel(
    n_dp, n_tp, pack,
    attn, ograd, proj_in, proj_out, targets, out,
    a_buf, g_buf, wi, wo, t_buf, rs_out, rs_in, a2a_out, a2a_in, s_all,
    gram, cz, c_all, c_mat, inv_ref,
    load_sem, rs_s, rs_r, a2a_s, a2a_r, ag_s, ag_r, gr_s, gr_r, cz_s, cz_r, ca_s, ca_r,
):
    d, z = lax.axis_index("dp"), lax.axis_index("tensor")
    share = rs_out.shape[1]
    rank = proj_in.shape[0]
    per = s_all.shape[0] // n_dp
    n = s_all.shape[0]
    half = s_all.shape[1]
    slots = a2a_out.shape[1] // half

    def each(count, body):
        if count <= 16:
            for k in range(1, count):
                body(k)
        else:
            lax.fori_loop(1, count, lambda k, c: (body(k), c)[1], 0)

    def z_peer(k):
        return lax.rem(z + k, n_tp)

    def d_peer(k):
        return lax.rem(d + k, n_dp)

    barrier = pltpu.get_barrier_semaphore()
    each(n_tp, lambda k: pl.semaphore_signal(barrier, inc=1, device_id=(d, z_peer(k)), device_id_type=MESH))
    each(n_dp, lambda k: pl.semaphore_signal(barrier, inc=1, device_id=(d_peer(k), z), device_id_type=MESH))

    load_pi = pltpu.make_async_copy(proj_in, wi.at[pl.ds(0, rank)], load_sem.at[0])
    load_po = pltpu.make_async_copy(proj_out, wo.at[pl.ds(rank, rank)], load_sem.at[1])
    load_pi.start()
    load_po.start()
    order = [k for k in (2, 3, 1) if k < n_tp] + list(range(4, n_tp)) + [0]
    loads = {}
    for k in order:
        rows = pl.ds(pl.multiple_of(z_peer(k) * share, share), share)
        loads[k] = (
            pltpu.make_async_copy(attn.at[rows], a_buf.at[k], load_sem.at[3 + 2 * k]),
            pltpu.make_async_copy(ograd.at[rows], g_buf.at[k], load_sem.at[4 + 2 * k]),
        )
        for copy in loads[k]:
            copy.start()
    load_t = pltpu.make_async_copy(targets, t_buf, load_sem.at[2])
    load_t.start()
    wi[pl.ds(rank, rank), :] = jnp.zeros((rank, wi.shape[1]), wi.dtype)
    wo[pl.ds(0, rank), :] = jnp.zeros((rank, wo.shape[1]), wo.dtype)
    load_pi.wait()
    load_po.wait()

    def z_copy(src, dst, send, recv, k):
        return pltpu.make_async_remote_copy(
            src_ref=src, dst_ref=dst, send_sem=send, recv_sem=recv,
            device_id=(d, z_peer(k)), device_id_type=MESH,
        )

    def d_copy(src, dst, send, recv, k):
        return pltpu.make_async_remote_copy(
            src_ref=src, dst_ref=dst, send_sem=send, recv_sem=recv,
            device_id=(d_peer(k), z), device_id_type=MESH,
        )

    sends = []

    def rs_copy(k):
        return z_copy(rs_out.at[k], rs_in.at[z], rs_s.at[k], rs_r.at[z], k)

    for position, k in enumerate(order):
        for copy in loads[k]:
            copy.wait()
        part = lax.dot_general(a_buf[k], wi[...], NT, preferred_element_type=jnp.float32)
        part = part + lax.dot_general(g_buf[k], wo[...], NT, preferred_element_type=jnp.float32)
        if k:
            rs_out[k] = part
            if position == 0:
                pl.semaphore_wait(barrier, n_tp + n_dp - 2)
            copy = rs_copy(k)
            copy.start()
            sends.append(copy)
        else:
            rs_in[z] = part

    def wait_z(buf, recv):
        for k in range(1, n_tp):
            src = lax.rem(z + n_tp - k, n_tp)
            pltpu.make_async_remote_copy(
                src_ref=buf.at[src], dst_ref=buf.at[src], send_sem=recv.at[src], recv_sem=recv.at[src],
                device_id=(d, src), device_id_type=MESH,
            ).wait_recv()

    wait_z(rs_in, rs_r)
    low = rs_in[0]
    for src in range(1, n_tp):
        low = low + rs_in[src]
    lanes = lax.broadcasted_iota(jnp.int32, low.shape, 1)
    grads = jnp.where(lanes < rank, pltpu.roll(low, rank, 1), low)
    inputs_t = low.T[:rank]
    token = lax.broadcasted_iota(jnp.int32, inputs_t.shape, 1) + z * share
    first = (z * share) // LEN
    left = jnp.concatenate(
        [
            jnp.where((token >= (first + s) * LEN) & (token < (first + s + 1) * LEN), inputs_t, 0.0)
            for s in range(slots)
        ],
        axis=0,
    )
    prods = dot32(left, grads, NN)
    low_lanes = lax.broadcasted_iota(jnp.int32, (half, 2 * rank), 1) < rank
    for q in range(n_tp):
        for s in range(slots):
            base = s * rank + q * 2 * half
            a2a_out[q, s * half : (s + 1) * half, :] = jnp.where(
                low_lanes, prods[base : base + half], prods[base + half : base + 2 * half]
            )
    for k in range(1, n_tp):
        copy = z_copy(a2a_out.at[z_peer(k)], a2a_in.at[z], a2a_s.at[k], a2a_r.at[z], k)
        copy.start()
        sends.append(copy)
    a2a_in[z] = a2a_out[z]
    wait_z(a2a_in, a2a_r)
    mine = [None] * per
    for src in range(n_tp):
        for s in range(slots):
            sample = (src * share) // LEN + s
            if sample * LEN >= (src + 1) * share:
                continue
            term = a2a_in[src, s * half : (s + 1) * half, :]
            mine[sample] = term if mine[sample] is None else mine[sample] + term
    for sample in range(per):
        s_all[d * per + sample] = mine[sample]

    own = pl.ds(d * per, per)

    def ag_copy(k):
        return d_copy(s_all.at[own], s_all.at[own], ag_s.at[k], ag_r.at[d], k)

    each(n_dp, lambda k: ag_copy(k).start())

    own_flat = jnp.concatenate([s_all[own, r, :] for r in range(half)], axis=1)
    load_t.wait()
    target_cols = jnp.concatenate([t_buf[i] for r in range(half) for i in (r, r + half)], axis=0)
    cz[z, pl.ds(0, per), :] = dot32(own_flat, target_cols, NN)
    if cz.shape[1] > per:
        cz[z, pl.ds(per, cz.shape[1] - per), :] = jnp.zeros((cz.shape[1] - per, cz.shape[2]), jnp.float32)
    for k in range(1, n_tp):
        copy = z_copy(cz.at[z], cz.at[z], cz_s.at[k], cz_r.at[z], k)
        copy.start()
        sends.append(copy)

    def wait_ag(k):
        src = lax.rem(d + n_dp - k, n_dp)
        block = s_all.at[pl.ds(src * per, per)]
        pltpu.make_async_remote_copy(
            src_ref=block, dst_ref=block, send_sem=ag_r.at[src], recv_sem=ag_r.at[src],
            device_id=(src, z), device_id_type=MESH,
        ).wait_recv()

    each(n_dp, wait_ag)
    flat = jnp.concatenate([s_all[:, r, :] for r in range(half)], axis=1)
    width = gram.shape[2]
    if pack:
        pad = jnp.zeros((width // 2 - n, flat.shape[1]), jnp.float32)
        full = dot32(flat, jnp.concatenate([flat, pad, flat, pad], axis=0), NT)
        g_lanes = lax.broadcasted_iota(jnp.int32, (n // 2, width), 1)
        gram[z] = jnp.where(g_lanes < width // 2, full[: n // 2], full[n // 2 :])
    else:
        gram[z] = dot32(flat, flat, NT)
    for k in range(1, n_tp):
        copy = z_copy(gram.at[z], gram.at[z], gr_s.at[k], gr_r.at[z], k)
        copy.start()
        sends.append(copy)

    wait_z(cz, cz_r)
    total = cz[0]
    for src in range(1, n_tp):
        total = total + cz[src]
    c_all[d] = total

    def ca_copy(k):
        return d_copy(c_all.at[d], c_all.at[d], ca_s.at[k], ca_r.at[d], k)

    each(n_dp, lambda k: ca_copy(k).start())

    wait_z(gram, gr_r)
    g_sum = gram[0]
    for src in range(1, n_tp):
        g_sum = g_sum + gram[src]
    if pack:
        g_sum = jnp.concatenate([g_sum, pltpu.roll(g_sum, width // 2, 1)], axis=0)
        system_width = width // 2
        wide = g_sum
    else:
        system_width = width
        wide = jnp.concatenate([g_sum, jnp.zeros_like(g_sum)], axis=1)
    g_rows = lax.broadcasted_iota(jnp.int32, wide.shape, 0)
    g_cols = lax.broadcasted_iota(jnp.int32, wide.shape, 1)
    wide = jnp.where(g_cols < n, wide, 0.0)
    diagonal = g_rows == g_cols
    trace = jnp.sum(jnp.where(diagonal, wide, 0.0))
    damping = damping_ratio * trace / (n * rank * rank) + epsilon
    system = wide / n + jnp.where(diagonal, damping, 0.0)
    inverse = invert(system, n, system_width, inv_ref)
    inv_ref[:, pl.ds(0, system_width)] = inverse

    def wait_ca(k):
        src = lax.rem(d + n_dp - k, n_dp)
        block = c_all.at[src]
        pltpu.make_async_remote_copy(
            src_ref=block, dst_ref=block, send_sem=ca_r.at[src], recv_sem=ca_r.at[src],
            device_id=(src, z), device_id_type=MESH,
        ).wait_recv()

    each(n_dp, wait_ca)
    for q in range(n_dp):
        c_mat[q * per : (q + 1) * per, :] = c_all[q, :per, :]
    weights = jnp.concatenate([inv_ref[pl.ds(d * per + i, 1), :] for i in range(per)], axis=0)[:, :n]
    out[...] = dot32(weights, c_mat[...], NN)

    for copy in sends:
        copy.wait_send()
    each(n_dp, lambda k: ag_copy(k).wait_send())
    each(n_dp, lambda k: ca_copy(k).wait_send())


def shards(n_dp, n_tp, attn_out, out_grad, proj_in, proj_out, targets):
    tokens, model = attn_out.shape
    rank = proj_in.shape[0]
    n_targets, part_width, _ = targets.shape
    per = tokens // LEN
    n = per * n_dp
    share = tokens // n_tp
    half = part_width // 2
    slots = max(-(-((q + 1) * share) // LEN) - (q * share) // LEN for q in range(n_tp))
    pack = n <= rank and n % 16 == 0 and rank == 64
    padded = -(-per // 8) * 8
    gram_shape = (n_tp, n // 2, 2 * rank) if pack else (n_tp, n, n)
    inv_width = 2 * rank if pack else 2 * n
    f32, dma = jnp.float32, pltpu.SemaphoreType.DMA
    any_spec = pl.BlockSpec(memory_space=pl.ANY)
    return pl.pallas_call(
        functools.partial(kernel, n_dp, n_tp, pack),
        out_shape=jax.ShapeDtypeStruct((per, n_targets), f32),
        in_specs=[any_spec] * 5,
        out_specs=pl.BlockSpec(memory_space=pltpu.VMEM),
        scratch_shapes=[
            pltpu.VMEM((n_tp, share, model), attn_out.dtype),
            pltpu.VMEM((n_tp, share, model), out_grad.dtype),
            pltpu.VMEM((2 * rank, model), proj_in.dtype),
            pltpu.VMEM((2 * rank, model), proj_out.dtype),
            pltpu.VMEM((part_width, rank, n_targets), f32),
            pltpu.VMEM((n_tp, share, 2 * rank), f32),
            pltpu.VMEM((n_tp, share, 2 * rank), f32),
            pltpu.VMEM((n_tp, slots * half, 2 * rank), f32),
            pltpu.VMEM((n_tp, slots * half, 2 * rank), f32),
            pltpu.VMEM((n, half, 2 * rank), f32),
            pltpu.VMEM(gram_shape, f32),
            pltpu.VMEM((n_tp, padded, n_targets), f32),
            pltpu.VMEM((n_dp, padded, n_targets), f32),
            pltpu.VMEM((n, n_targets), f32),
            pltpu.VMEM((n, inv_width), f32),
            dma((3 + 2 * n_tp,)),
        ]
        + [dma((n_tp,))] * 4
        + [dma((n_dp,))] * 2
        + [dma((n_tp,))] * 4
        + [dma((n_dp,))] * 2,
        compiler_params=pltpu.CompilerParams(
            collective_id=0, has_side_effects=True, vmem_limit_bytes=60 * 1024 * 1024
        ),
    )(attn_out, out_grad, proj_in, proj_out, jnp.transpose(targets, (1, 2, 0)))


def solution(mesh):
    in_specs = (
        P("dp", "tensor"),
        P("dp", "tensor"),
        P(None, "tensor"),
        P(None, "tensor"),
        P(None, "tensor", None),
    )
    return jax.shard_map(
        functools.partial(shards, mesh.shape["dp"], mesh.shape["tensor"]),
        mesh=mesh, in_specs=in_specs, out_specs=P("dp", None), check_vma=False,
    )
```
